32 devices in a mesh: rows: 8 (over y, x, core), tp: 4 (over z).
Axes of the slice: x: 2, y: 2, z: 4, core: 2. Of those that a mesh axis runs over, the one named last changes fastest.
Arguments:
- train_up: bfloat16 [5120, 20480], P('rows', 'tp'), may hold values from -0.078125 to 0.078125
- low_up: bfloat16 [5120, 16], P('rows'), may hold values from -0.078125 to 0.078125
- high_up: bfloat16 [16, 20480], P(None, 'tp'), may hold values from -1.5 to 1.5
- norm_train: float32 [5120], P(('rows', 'tp')), may hold values from 0.25 to 1.75
- norm_step: float32 [5120], P(('rows', 'tp')), may hold values from -0.3 to 0.3
Outputs:
- ready_up: bfloat16 [20480, 5120], P('tp')
- serve_norm: bfloat16 [5120], replicated
The draws below stay inside these ranges and needn't reach their ends.
All inputs are finite; a program needn't handle non-finite values.
Results may differ from the reference program's by a relative error of at most 0.001.
Values may be sent and summed in bfloat16 or wider, within the bound.
A program may use at most 192 MiB of HBM per device.

```python
import jax
import jax.numpy as jnp

D_MODEL = 5120
D_INNER = 20480
RANK = 16


def shard_levels(own_key, extent, shards, smallest, high):
    def one(position, blocks):
        heights = jax.random.uniform(jax.random.fold_in(jax.random.fold_in(own_key, 6), position), (blocks,), jnp.float32, smallest / len(shards), high / len(shards))
        return jnp.repeat(jnp.exp(heights), extent[position] // blocks).reshape((-1,) + (1,) * (len(extent) - position - 1))

    level = one(*shards[0])
    for cut in shards[1:]:
        level = level * one(*cut)
    return level


def scatter_about(own_key, extent, deviation, limit, shards=(), dtype=jnp.bfloat16):
    result = jax.random.normal(own_key, extent, jnp.float32) * deviation
    if len(shards) > 0:
        result = shard_levels(own_key, extent, shards, -0.22, 0.18) * result
    return jnp.clip(result, min=-limit, max=limit).astype(dtype)


def setup_inputs(seed: int = 0) -> dict:
    keys = jax.random.split(jax.random.key(seed), 6)
    return {
        "train_up": scatter_about(keys[0], (D_MODEL, D_INNER), D_MODEL ** -0.5, 0.078125, ((0, 8), (1, 4))),
        "low_up": scatter_about(keys[1], (D_MODEL, RANK), D_MODEL ** -0.5, 0.078125, ((0, 8),)),
        "high_up": scatter_about(keys[2], (RANK, D_INNER), RANK ** -0.5, 1.5, ((1, 4),)),
        "norm_train": jnp.clip(1.0 + 0.15 * jax.random.normal(keys[3], (D_MODEL,), jnp.float32), 0.25, 1.75),
        "norm_step": jnp.clip(jax.random.uniform(keys[4], (D_MODEL,), jnp.float32, -0.3, 0.3) * shard_levels(keys[4], (D_MODEL,), ((0, 32),), -0.4, 0.0), -0.3, 0.3),
    }


mix_rate = 2.0


def reference(train_up, low_up, high_up, norm_train, norm_step):
    latest_up = train_up.astype(jnp.float32) + mix_rate * jnp.dot(low_up, high_up, preferred_element_type=jnp.float32)
    ready_up = latest_up.T.astype(jnp.bfloat16)
    serve_norm = (norm_train + norm_step).astype(jnp.bfloat16)
    return ready_up, serve_norm
```

```python
import functools

import jax
import jax.numpy as jnp
from jax import lax
from jax.experimental import pallas as pl
from jax.experimental.pallas import tpu as pltpu
from jax.sharding import PartitionSpec as P


mix_rate = 2.0
PIECES = 8
ANY = pl.BlockSpec(memory_space=pl.ANY)


def merge_kernel(train_ref, low_ref, high_ref, norm_ref, *refs, tile):
    piece_ref = refs[-1]
    rows = train_ref.shape[1]
    for start in range(0, rows, tile):
        cols = slice(start, start + tile)
        update = lax.dot_general(
            high_ref[:, cols], low_ref[...], (((0,), (0,)), ((), ())), preferred_element_type=jnp.float32
        )
        latest = train_ref[:, cols].T.astype(jnp.float32) + mix_rate * update
        piece_ref[cols, :] = latest.astype(jnp.bfloat16)
    if piece_ref.shape[0] > rows:
        piece_ref[rows:, :] = jnp.broadcast_to(norm_ref[...], (piece_ref.shape[0] - rows, norm_ref.shape[1]))


def merge_piece(train, low, high, norm, index, rows, extra, after):
    rank, width = low.shape
    return pl.pallas_call(
        functools.partial(merge_kernel, tile=128),
        grid=(1,),
        in_specs=[
            pl.BlockSpec((width, rows), lambda i: (0, index)),
            pl.BlockSpec((rank, width), lambda i: (0, 0)),
            pl.BlockSpec((rank, rows), lambda i: (0, index)),
            pl.BlockSpec((1, width), lambda i: (0, 0)),
        ] + [ANY] * len(after),
        out_specs=pl.BlockSpec((rows + extra, width), lambda i: (0, 0)),
        out_shape=jax.ShapeDtypeStruct((rows + extra, width), jnp.bfloat16),
        cost_estimate=pl.CostEstimate(
            flops=2 * width * rank * rows, bytes_accessed=4 * width * rows, transcendentals=0
        ),
    )(train, low, high, norm, *after)


def flip(position, mask):
    bit = 1
    while bit <= mask:
        if mask & bit:
            position = position + bit - 2 * bit * ((position // bit) % 2)
        bit *= 2
    return position


def place_kernel(*refs, count, slots, rows, width, inputs):
    pieces = refs[:count]
    out = refs[inputs]
    buffer, in_sem, out_sem = refs[-3:]
    me = lax.axis_index("rows")

    def load(i):
        return pltpu.make_async_copy(pieces[i].at[pl.ds(0, rows), :], buffer.at[i], in_sem.at[i])

    def store(i):
        index, mask = slots[i]
        column = pl.multiple_of(flip(me, mask) * width, width)
        return pltpu.make_async_copy(
            buffer.at[i], out.at[pl.ds(index * rows, rows), pl.ds(column, width)], out_sem.at[i]
        )

    for i in range(count):
        load(i).start()
    for i in range(count):
        load(i).wait()
        store(i).start()
    for i in range(count):
        store(i).wait()


def place(out, pieces, slots, rows, width, shape):
    count = len(pieces)
    if width % 128:
        me = lax.axis_index("rows")
        out = jnp.zeros(shape, jnp.bfloat16) if out is None else out
        for piece, (index, mask) in zip(pieces, slots):
            out = lax.dynamic_update_slice(out, piece[:rows], (index * rows, flip(me, mask) * width))
        return out
    aliased = out is not None
    operands = list(pieces) + ([out] if aliased else [])
    return pl.pallas_call(
        functools.partial(
            place_kernel, count=count, slots=tuple(slots), rows=rows, width=width, inputs=len(operands)
        ),
        in_specs=[ANY] * len(operands),
        out_specs=ANY,
        out_shape=jax.ShapeDtypeStruct(shape, jnp.bfloat16),
        scratch_shapes=[
            pltpu.VMEM((count, rows, width), jnp.bfloat16),
            pltpu.SemaphoreType.DMA((count,)),
            pltpu.SemaphoreType.DMA((count,)),
        ],
        input_output_aliases={count: 0} if aliased else {},
        cost_estimate=pl.CostEstimate(flops=0, bytes_accessed=4 * count * rows * width, transcendentals=0),
    )(*operands)


def add_norm(train, step, after):
    def kernel(train_ref, step_ref, *refs):
        refs[-1][...] = (train_ref[...] + step_ref[...]).astype(jnp.bfloat16)

    vmem = pl.BlockSpec(memory_space=pltpu.VMEM)
    return pl.pallas_call(
        kernel,
        in_specs=[vmem, vmem] + [ANY] * len(after),
        out_specs=vmem,
        out_shape=jax.ShapeDtypeStruct((1, train.shape[0]), jnp.bfloat16),
        name="add_norm",
    )(train[None, :], step[None, :], *after)


def collect_norm(pieces, rows, n, width):
    if width % 128:
        gains = jnp.stack([piece[rows] for piece in pieces])
        return gains[lax.axis_index("rows") ^ jnp.arange(n)].reshape(1, -1)

    def kernel(*refs):
        out, buffer, sem = refs[n:]
        me = lax.axis_index("rows")
        copies = [
            pltpu.make_async_copy(refs[k].at[pl.ds(rows, 16), :], buffer.at[k], sem.at[k]) for k in range(n)
        ]
        for copy in copies:
            copy.start()
        for k, copy in enumerate(copies):
            copy.wait()
            column = pl.multiple_of(flip(me, k) * width, 128)
            out[:, pl.ds(column, width)] = buffer[k, 0:1, :]

    return pl.pallas_call(
        kernel,
        in_specs=[ANY] * n,
        out_specs=pl.BlockSpec(memory_space=pltpu.VMEM),
        out_shape=jax.ShapeDtypeStruct((1, n * width), jnp.bfloat16),
        scratch_shapes=[pltpu.VMEM((n, 16, width), jnp.bfloat16), pltpu.SemaphoreType.DMA((n,))],
        name="collect_norm",
    )(*pieces)


def per_device(train_up, low_up, high_up, norm_train, norm_step, *, n, t):
    width, m = train_up.shape
    pieces = max(p for p in range(1, PIECES + 1) if m % (128 * p) == 0)
    rows = m // pieces
    pairs = [list(range(i, min(i + 2, pieces))) for i in range(0, pieces, 2)]
    outer = [1 << b for b in range(1, n.bit_length() - 1)]
    low_up = low_up.T

    def swap(x, axis, size, mask):
        return lax.ppermute(x, axis, [(i, i ^ mask) for i in range(size)])

    def gather_norm(after):
        norm = add_norm(norm_train, norm_step, after)
        mine = lax.axis_index("tp")
        bit = 1
        while bit < t:
            other = swap(norm, "tp", t, bit)
            upper = (mine // bit) % 2 == 1
            norm = jnp.where(
                upper,
                jnp.concatenate([other, norm], axis=1),
                jnp.concatenate([norm, other], axis=1),
            )
            bit *= 2
        return norm

    dummy = jnp.zeros((1, width), jnp.bfloat16)
    norm_pair = max(len(pairs) - 2, 0)
    carrier = pairs[norm_pair][-1]
    held = {}
    for index in range(pieces):
        extra = 16 if index == carrier else 0
        norm = gather_norm([]) if extra else dummy
        held[index] = {0: merge_piece(train_up, low_up, high_up, norm, index, rows, extra, [])}

    early, late = [], []
    for pair in pairs:
        first, second = [], []
        for index in pair:
            have = held[index]
            k = index % max(len(outer), 1)
            order = outer[k:] + outer[:k]
            first.append((index, 0))
            for step, bit in enumerate(order):
                for mask in list(have):
                    final = step == len(order) - 1 and mask != 0
                    have[mask ^ bit] = swap(have[mask], "rows", n, bit)
                    (second if final else first).append((index, mask ^ bit))
        for group in (first, second):
            for index, mask in list(group):
                held[index][mask ^ 1] = swap(held[index][mask], "rows", n, 1)
                group.append((index, mask ^ 1))
        early.append(first)
        late.append(second)

    out = None
    for groups in (early, late):
        for group in groups:
            if group:
                out = place(out, [held[i][k] for i, k in group], group, rows, width, (m, n * width))
    serve_norm = collect_norm([held[carrier][k] for k in range(n)], rows, n, width)
    return out, serve_norm.reshape(-1)


def solution(mesh):
    placed = (P("rows", "tp"), P("rows", None), P(None, "tp"), P(("rows", "tp")), P(("rows", "tp")))
    body = functools.partial(per_device, n=mesh.shape["rows"], t=mesh.shape["tp"])
    return jax.shard_map(
        body, mesh=mesh, in_specs=placed, out_specs=(P("tp", None), P()), check_vma=False
    )
```

```python
import functools

import jax
import jax.numpy as jnp
from jax import lax
from jax.experimental import pallas as pl
from jax.experimental.pallas import tpu as pltpu
from jax.sharding import PartitionSpec as P


mix_rate = 2.0
PIECES = 8
ANY = pl.BlockSpec(memory_space=pl.ANY)


def merge_kernel(train_ref, low_ref, high_ref, *refs, tile):
    piece_ref = refs[-1]
    rows = train_ref.shape[1]
    for start in range(0, rows, tile):
        cols = slice(start, start + tile)
        update = lax.dot_general(
            high_ref[:, cols], low_ref[...], (((0,), (0,)), ((), ())), preferred_element_type=jnp.float32
        )
        latest = train_ref[:, cols].T.astype(jnp.float32) + mix_rate * update
        piece_ref[cols, :] = latest.astype(jnp.bfloat16)
    if len(refs) > 1:
        norm_ref = refs[0]
        piece_ref[rows:, :] = jnp.broadcast_to(norm_ref[...], (piece_ref.shape[0] - rows, norm_ref.shape[1]))


def merge_piece(train, low, high, norm, index, rows):
    extra = 0 if norm is None else 16
    rank, width = low.shape
    return pl.pallas_call(
        functools.partial(merge_kernel, tile=128),
        grid=(1,),
        in_specs=[
            pl.BlockSpec((width, rows), lambda i: (0, index)),
            pl.BlockSpec((rank, width), lambda i: (0, 0)),
            pl.BlockSpec((rank, rows), lambda i: (0, index)),
        ] + ([] if norm is None else [pl.BlockSpec((1, width), lambda i: (0, 0))]),
        out_specs=pl.BlockSpec((rows + extra, width), lambda i: (0, 0)),
        out_shape=jax.ShapeDtypeStruct((rows + extra, width), jnp.bfloat16),
        cost_estimate=pl.CostEstimate(
            flops=2 * width * rank * rows, bytes_accessed=4 * width * rows, transcendentals=0
        ),
    )(train, low, high, *([] if norm is None else [norm]))


def flip(position, mask):
    bit = 1
    while bit <= mask:
        if mask & bit:
            position = position + bit - 2 * bit * ((position // bit) % 2)
        bit *= 2
    return position


def place_kernel(*refs, count, slots, rows, width, inputs):
    pieces = refs[:count]
    out = refs[inputs]
    buffer, in_sem, out_sem = refs[-3:]
    me = lax.axis_index("rows")

    def load(i):
        return pltpu.make_async_copy(pieces[i].at[pl.ds(0, rows), :], buffer.at[i], in_sem.at[i])

    def store(i):
        index, mask = slots[i]
        column = pl.multiple_of(flip(me, mask) * width, width)
        return pltpu.make_async_copy(
            buffer.at[i], out.at[pl.ds(index * rows, rows), pl.ds(column, width)], out_sem.at[i]
        )

    for i in range(count):
        load(i).start()
    for i in range(count):
        load(i).wait()
        store(i).start()
    for i in range(count):
        store(i).wait()


def place(out, pieces, slots, rows, width, shape):
    count = len(pieces)
    if width % 128:
        me = lax.axis_index("rows")
        out = jnp.zeros(shape, jnp.bfloat16) if out is None else out
        for piece, (index, mask) in zip(pieces, slots):
            out = lax.dynamic_update_slice(out, piece[:rows], (index * rows, flip(me, mask) * width))
        return out
    aliased = out is not None
    operands = list(pieces) + ([out] if aliased else [])
    return pl.pallas_call(
        functools.partial(
            place_kernel, count=count, slots=tuple(slots), rows=rows, width=width, inputs=len(operands)
        ),
        in_specs=[ANY] * len(operands),
        out_specs=ANY,
        out_shape=jax.ShapeDtypeStruct(shape, jnp.bfloat16),
        scratch_shapes=[
            pltpu.VMEM((count, rows, width), jnp.bfloat16),
            pltpu.SemaphoreType.DMA((count,)),
            pltpu.SemaphoreType.DMA((count,)),
        ],
        input_output_aliases={count: 0} if aliased else {},
        cost_estimate=pl.CostEstimate(flops=0, bytes_accessed=4 * count * rows * width, transcendentals=0),
    )(*operands)


def add_norm(train, step):
    def kernel(train_ref, step_ref, out_ref):
        out_ref[...] = (train_ref[...] + step_ref[...]).astype(jnp.bfloat16)

    vmem = pl.BlockSpec(memory_space=pltpu.VMEM)
    return pl.pallas_call(
        kernel,
        in_specs=[vmem, vmem],
        out_specs=vmem,
        out_shape=jax.ShapeDtypeStruct((1, train.shape[0]), jnp.bfloat16),
        name="add_norm",
    )(train[None, :], step[None, :])


def collect_norm(pieces, rows, n, width):
    if width % 128:
        gains = jnp.stack([piece[rows] for piece in pieces])
        return gains[lax.axis_index("rows") ^ jnp.arange(n)].reshape(1, -1)

    def kernel(*refs):
        out, buffer, sem = refs[n:]
        me = lax.axis_index("rows")
        copies = [
            pltpu.make_async_copy(refs[k].at[pl.ds(rows, 16), :], buffer.at[k], sem.at[k]) for k in range(n)
        ]
        for copy in copies:
            copy.start()
        for k, copy in enumerate(copies):
            copy.wait()
            column = pl.multiple_of(flip(me, k) * width, 128)
            out[:, pl.ds(column, width)] = buffer[k, 0:1, :]

    return pl.pallas_call(
        kernel,
        in_specs=[ANY] * n,
        out_specs=pl.BlockSpec(memory_space=pltpu.VMEM),
        out_shape=jax.ShapeDtypeStruct((1, n * width), jnp.bfloat16),
        scratch_shapes=[pltpu.VMEM((n, 16, width), jnp.bfloat16), pltpu.SemaphoreType.DMA((n,))],
        name="collect_norm",
    )(*pieces)


def per_device(train_up, low_up, high_up, norm_train, norm_step, *, n, t):
    width, m = train_up.shape
    pieces = max(p for p in range(1, PIECES + 1) if m % (128 * p) == 0)
    rows = m // pieces
    pairs = [list(range(i, min(i + 2, pieces))) for i in range(0, pieces, 2)]
    outer = [1 << b for b in range(1, n.bit_length() - 1)]
    low_up = low_up.T

    def swap(x, axis, size, mask):
        return lax.ppermute(x, axis, [(i, i ^ mask) for i in range(size)])

    def gather_norm():
        norm = add_norm(norm_train, norm_step)
        mine = lax.axis_index("tp")
        bit = 1
        while bit < t:
            other = swap(norm, "tp", t, bit)
            upper = (mine // bit) % 2 == 1
            norm = jnp.where(
                upper,
                jnp.concatenate([other, norm], axis=1),
                jnp.concatenate([norm, other], axis=1),
            )
            bit *= 2
        return norm

    norm_pair = max(len(pairs) - 2, 0)
    carrier = pairs[norm_pair][-1]
    held = {}
    for index in range(pieces):
        norm = gather_norm() if index == carrier else None
        held[index] = {0: merge_piece(train_up, low_up, high_up, norm, index, rows)}

    early, late = [], []
    for pair in pairs:
        first, second = [], []
        for index in pair:
            have = held[index]
            k = index % max(len(outer), 1)
            order = outer[k:] + outer[:k]
            first.append((index, 0))
            for step, bit in enumerate(order):
                for mask in list(have):
                    final = step == len(order) - 1 and mask != 0
                    have[mask ^ bit] = swap(have[mask], "rows", n, bit)
                    (second if final else first).append((index, mask ^ bit))
        for group in (first, second):
            for index, mask in list(group):
                held[index][mask ^ 1] = swap(held[index][mask], "rows", n, 1)
                group.append((index, mask ^ 1))
        early.append(first)
        late.append(second)

    out = None
    for groups in (early, late):
        for group in groups:
            if group:
                out = place(out, [held[i][k] for i, k in group], group, rows, width, (m, n * width))
    serve_norm = collect_norm([held[carrier][k] for k in range(n)], rows, n, width)
    return out, serve_norm.reshape(-1)


def solution(mesh):
    placed = (P("rows", "tp"), P("rows", None), P(None, "tp"), P(("rows", "tp")), P(("rows", "tp")))
    body = functools.partial(per_device, n=mesh.shape["rows"], t=mesh.shape["tp"])
    return jax.shard_map(
        body, mesh=mesh, in_specs=placed, out_specs=(P("tp", None), P()), check_vma=False
    )
```
